32 devices in a mesh: dp: 16 (over z, y, core), seq: 2 (over x).
Axes of the slice: x: 2, y: 2, z: 4, core: 2. Of those that a mesh axis runs over, the one named last changes fastest.
Arguments:
- tokens: bfloat16 [17664, 1024], P(('dp', 'seq')), may hold values from -6 to 6
- skipped: bfloat16 [17664, 1024], P(('dp', 'seq')), may hold values from -6 to 6
- cotangent: bfloat16 [17664, 1024], P(('dp', 'seq')), may hold values from -6 to 6
- merge_weight: bfloat16 [2048, 1024], P('dp'), may hold values from -0.125 to 0.125
- merge_bias: bfloat16 [1024], P('dp'), may hold values from -2 to 2
- first_gain: bfloat16 [1024], P('dp'), may hold values from 0.099609375 to 1.8984375
- first_shift: bfloat16 [1024], P('dp'), may hold values from -2 to 2
- project_in: bfloat16 [1024, 3072], P('dp'), may hold values from -0.1875 to 0.1875
- project_out: bfloat16 [1024, 1024], P('dp'), may hold values from -1.5 to 1.5
- project_bias: bfloat16 [1024], P('dp'), may hold values from -2 to 2
- second_gain: bfloat16 [1024], P('dp'), may hold values from 0.099609375 to 1.8984375
- second_shift: bfloat16 [1024], P('dp'), may hold values from -2 to 2
- expand_weight: bfloat16 [1024, 4096], P('dp'), may hold values from -0.1875 to 0.1875
- expand_bias: bfloat16 [4096], P('dp'), may hold values from -2 to 2
- reduce_weight: bfloat16 [4096, 1024], P('dp'), may hold values from -0.09375 to 0.09375
- reduce_bias: bfloat16 [1024], P('dp'), may hold values from -2 to 2
Outputs:
- output: bfloat16 [17664, 1024], P(('dp', 'seq'))
- tokens_grad: float32 [17664, 1024], P(('dp', 'seq'))
- skipped_grad: float32 [17664, 1024], P(('dp', 'seq'))
- merge_weight_grad: float32 [2048, 1024], P('dp')
- project_in_grad: float32 [1024, 3072], P('dp')
- project_out_grad: float32 [1024, 1024], P('dp')
- expand_weight_grad: float32 [1024, 4096], P('dp')
- reduce_weight_grad: float32 [4096, 1024], P('dp')
- merge_bias_grad: float32 [1024], P('dp')
- first_gain_grad: float32 [1024], P('dp')
- first_shift_grad: float32 [1024], P('dp')
- project_bias_grad: float32 [1024], P('dp')
- second_gain_grad: float32 [1024], P('dp')
- second_shift_grad: float32 [1024], P('dp')
- expand_bias_grad: float32 [4096], P('dp')
- reduce_bias_grad: float32 [1024], P('dp')
The draws below stay inside these ranges and needn't reach their ends.
All inputs are finite; a program needn't handle non-finite values.
Results may differ from the reference program's by a relative error of at most 0.012.
Values may be sent and summed in bfloat16 or wider, within the bound.
A program may use at most 320 MiB of HBM per device.

```python
import jax
import jax.numpy as jnp
from jax import lax

D = 1024
H = 16
HD = 64
FF = 4096
LEN = 1104
TOKENS = 17664


def levels(own_key, extent, shards, least, high):
    factor_of = 1.0
    for position, shards_of in shards:
        heights = jax.random.uniform(jax.random.fold_in(jax.random.fold_in(own_key, 6), position), (shards_of,), jnp.float32, least / len(shards), high / len(shards))
        factor_of = factor_of * jnp.repeat(jnp.exp(heights), extent[position] // shards_of).reshape((-1,) + (1,) * (len(extent) - 1 - position))
    return factor_of


def gaussian(stream_key, extent, deviation, bound, shards=(), held_as=jnp.bfloat16):
    values = deviation * jax.random.normal(stream_key, extent, jnp.float32)
    if shards:
        values = values * levels(stream_key, extent, shards, -0.22, 0.18)
    return jnp.clip(values, -bound, bound).astype(held_as)


def setup_inputs(seed: int = 0) -> dict:
    seeds = jax.random.split(jax.random.key(seed), 17)
    return {
        "tokens": gaussian(seeds[0], (TOKENS, D), 1.0, 6.0, ((0, 32),)),
        "skipped": gaussian(seeds[1], (TOKENS, D), 1.0, 6.0, ((0, 32),)),
        "cotangent": gaussian(seeds[2], (TOKENS, D), 1.0, 6.0, ((0, 32),)),
        "merge_weight": gaussian(seeds[3], (2 * D, D), (2 * D) ** -0.5, 0.125, ((0, 16),)),
        "merge_bias": gaussian(seeds[4], (D,), 0.3, 2.0, ((0, 16),)),
        "first_gain": jnp.clip(1.0 + 0.18 * jax.random.normal(seeds[5], (D,), jnp.float32), 0.099609375, 1.8984375).astype(jnp.bfloat16),
        "first_shift": gaussian(seeds[6], (D,), 0.3, 2.0, ((0, 16),)),
        "project_in": gaussian(seeds[7], (D, 3 * D), D ** -0.5, 0.1875, ((0, 16),)),
        "project_out": gaussian(seeds[8], (D, D), (max(1, D * 16 // LEN)) ** -0.5, 1.5, ((0, 16),)),
        "project_bias": gaussian(seeds[9], (D,), 0.3, 2.0, ((0, 16),)),
        "second_gain": jnp.clip(1.0 + 0.18 * jax.random.normal(seeds[10], (D,), jnp.float32), 0.099609375, 1.8984375).astype(jnp.bfloat16),
        "second_shift": gaussian(seeds[11], (D,), 0.3, 2.0, ((0, 16),)),
        "expand_weight": gaussian(seeds[12], (D, FF), D ** -0.5, 0.1875, ((0, 16),)),
        "expand_bias": gaussian(seeds[13], (FF,), 0.3, 2.0, ((0, 16),)),
        "reduce_weight": gaussian(seeds[14], (FF, D), FF ** -0.5, 0.09375, ((0, 16),)),
        "reduce_bias": gaussian(seeds[15], (D,), 0.3, 2.0, ((0, 16),)),
    }


@jax.custom_vjp
def low(v):
    return lax.optimization_barrier(v.astype(jnp.bfloat16)).astype(jnp.float32)

@jax.custom_vjp
def low_back(v):
    return v

def low_keep(v):
    return (low(v), None)

def low_pass(kept, grad):
    return (grad,)

def back_keep(v):
    return (v, None)

def back_low(kept, grad):
    return (low(grad),)
low.defvjp(low_keep, low_pass)
low_back.defvjp(back_keep, back_low)
EPSILON = 1e-05
HIGH = lax.Precision.HIGHEST

def matmul(left, right):
    return jnp.dot(left, right, precision=HIGH, preferred_element_type=jnp.float32)

def norm_apply(stream, gain, shift):
    centred = stream - lax.optimization_barrier(jnp.mean(stream, -1, keepdims=True))
    variance = lax.optimization_barrier(jnp.mean(centred * centred, -1, keepdims=True))
    return centred * lax.rsqrt(variance + EPSILON) * gain + shift

def block_forward(seq_tokens, seq_skip, params):
    merge_weight, merge_bias, first_gain, first_shift, project_in, project_out, project_bias, second_gain, second_shift, expand_weight, expand_bias, reduce_weight, reduce_bias = params
    joined = jnp.concatenate([seq_tokens, seq_skip], axis=1)
    stream = low_back(matmul(joined, merge_weight) + merge_bias)
    normed_one = low(norm_apply(stream, first_gain, first_shift))
    triple = low_back(low(matmul(normed_one, project_in)))
    triple = triple.reshape(LEN, 3, H, HD)
    queries = triple[:, 0]
    key_rows = triple[:, 1]
    values = triple[:, 2]
    scale = HD ** (-0.5)
    scores = jnp.einsum('qhd,khd->hqk', queries, key_rows, precision=HIGH) * scale
    scores = low_back(scores)
    probs = jax.nn.softmax(scores, axis=-1)
    attended = jnp.einsum('hqk,khd->qhd', low(probs), values, precision=HIGH).reshape(LEN, D)
    attended = low_back(low(attended))
    branch = low_back(matmul(attended, project_out) + project_bias)
    stream_two = stream + branch
    normed_two = low(norm_apply(stream_two, second_gain, second_shift))
    hidden_pre = low_back(matmul(normed_two, expand_weight) + expand_bias)
    activated = low(jax.nn.gelu(hidden_pre, approximate=False))
    mlp_out = low_back(matmul(activated, reduce_weight) + reduce_bias)
    return stream_two + mlp_out

def reference(tokens, skipped, cotangent, merge_weight, merge_bias, first_gain, first_shift, project_in, project_out, project_bias, second_gain, second_shift, expand_weight, expand_bias, reduce_weight, reduce_bias):
    params = tuple((item.astype(jnp.float32) for item in (merge_weight, merge_bias, first_gain, first_shift, project_in, project_out, project_bias, second_gain, second_shift, expand_weight, expand_bias, reduce_weight, reduce_bias)))
    count = tokens.shape[0] // LEN
    all_tokens = tokens.astype(jnp.float32).reshape(count, LEN, D)
    all_skip = skipped.astype(jnp.float32).reshape(count, LEN, D)
    all_cot = cotangent.astype(jnp.float32).reshape(count, LEN, D)

    def one_sequence(carry, pieces):
        piece_tokens, piece_skip, piece_cot = pieces
        result, backward = jax.vjp(block_forward, piece_tokens, piece_skip, params)
        grad_tokens, grad_skip, grad_params = backward(piece_cot)
        carry = jax.tree.map(jnp.add, carry, grad_params)
        return (carry, (result.astype(jnp.bfloat16), grad_tokens, grad_skip))
    zeros = jax.tree.map(jnp.zeros_like, params)
    sums, stacked = lax.scan(one_sequence, zeros, (all_tokens, all_skip, all_cot))
    outputs, grads_tok, grads_skip = stacked
    return (outputs.reshape(-1, D), grads_tok.reshape(-1, D), grads_skip.reshape(-1, D), sums[0], sums[4], sums[5], sums[9], sums[11], sums[1], sums[2], sums[3], sums[6], sums[7], sums[8], sums[10], sums[12])
```

```python
import functools
from functools import partial

import jax
import jax.numpy as jnp
from jax import lax
from jax.experimental import pallas as pl
from jax.experimental.pallas import tpu as pltpu
from jax.sharding import PartitionSpec as P

HD = 64
EPSILON = 1e-05
BF = jnp.bfloat16
FL = jnp.float32
MESHID = pl.DeviceIdType.MESH


def gather_kernel(Z, R, rc, L, shard, out, buf, lsem, su, ru, sd, rd, sy, ry, sx, rx, sc, rcv):
    n=R//rc
    hc=rc//2
    dp=lax.axis_index("dp"); s=lax.axis_index("seq")
    c=dp%2; y=(dp//2)%2; z=dp//4; h=s%2
    upd=(dp+4, s); dnd=(dp-4, s)
    yd=(dp+2-4*y, s); xd=(dp, s+1-2*h); cd=(dp+1-2*c, s)
    bar=pltpu.get_barrier_semaphore()
    has_up=z<Z-1; has_dn=z>0
    load=pltpu.make_async_copy(shard, buf, lsem.at[0]); load.start()
    @pl.when(has_up)
    def _(): pl.semaphore_signal(bar,inc=1,device_id=upd,device_id_type=MESHID)
    @pl.when(has_dn)
    def _(): pl.semaphore_signal(bar,inc=1,device_id=dnd,device_id_type=MESHID)
    for t in (yd,xd,cd): pl.semaphore_signal(bar,inc=1,device_id=t,device_id_type=MESHID)
    pl.semaphore_wait(bar,5-(z==0).astype(jnp.int32)-(z==Z-1).astype(jnp.int32))
    load.wait()
    store=pltpu.make_async_copy(buf, out.at[z,y,c], lsem.at[1]); store.start()
    def rows(k): return pl.ds(pl.multiple_of(k*rc,rc),rc)
    def half(k): return pl.ds(pl.multiple_of(k*rc+h*hc,hc),hc)
    def upc(d,k):
        src = buf.at[rows(k)] if d==0 else out.at[z-d,y,c,rows(k)]
        return pltpu.make_async_remote_copy(src, out.at[z-d,y,c,rows(k)], su.at[d,k], ru.at[d,k], device_id=upd, device_id_type=MESHID)
    def dnc(d,k):
        src = buf.at[rows(k)] if d==0 else out.at[z+d,y,c,rows(k)]
        return pltpu.make_async_remote_copy(src, out.at[z+d,y,c,rows(k)], sd.at[d,k], rd.at[d,k], device_id=dnd, device_id_type=MESHID)
    def ycp(k,mine):
        yy=y if mine else 1-y
        r=out.at[:,yy,c,half(k)]
        return pltpu.make_async_remote_copy(r,r,sy.at[k],ry.at[k],device_id=yd,device_id_type=MESHID)
    def xcp(k,mine):
        hh=half(k) if mine else pl.ds(pl.multiple_of(k*rc+(1-h)*hc,hc),hc)
        r=out.at[:,1-y,c,hh]
        return pltpu.make_async_remote_copy(r,r,sx.at[k],rx.at[k],device_id=xd,device_id_type=MESHID)
    def ccp(k,mine):
        r=out.at[:,:,c if mine else 1-c,rows(k)]
        return pltpu.make_async_remote_copy(r,r,sc.at[k],rcv.at[k],device_id=cd,device_id_type=MESHID)
    D=(Z-1)*L
    total=n+D+3*L
    def valid(k): return (k>=0)&(k<n)
    def body(t,_):
        for d in range(Z-1):
            k=t-d*L
            if d>0:
                @pl.when(valid(k)&(z>=d))
                def _():
                    pltpu.make_async_remote_copy(out.at[z-d,y,c,rows(k)],out.at[z-d,y,c,rows(k)],su.at[d-1,k],ru.at[d-1,k],device_id=dnd,device_id_type=MESHID).wait_recv()
                @pl.when(valid(k)&(z+d<=Z-1))
                def _():
                    pltpu.make_async_remote_copy(out.at[z+d,y,c,rows(k)],out.at[z+d,y,c,rows(k)],sd.at[d-1,k],rd.at[d-1,k],device_id=upd,device_id_type=MESHID).wait_recv()
            @pl.when(valid(k)&has_up&(z>=d))
            def _(): upc(d,k).start()
            @pl.when(valid(k)&has_dn&(z+d<=Z-1))
            def _(): dnc(d,k).start()
        d=Z-1
        k=t-D
        @pl.when(valid(k)&(z>=d))
        def _():
            pltpu.make_async_remote_copy(out.at[z-d,y,c,rows(k)],out.at[z-d,y,c,rows(k)],su.at[d-1,k],ru.at[d-1,k],device_id=dnd,device_id_type=MESHID).wait_recv()
        @pl.when(valid(k)&(z+d<=Z-1))
        def _():
            pltpu.make_async_remote_copy(out.at[z+d,y,c,rows(k)],out.at[z+d,y,c,rows(k)],sd.at[d-1,k],rd.at[d-1,k],device_id=upd,device_id_type=MESHID).wait_recv()
        @pl.when(k==0)
        def _(): store.wait()
        @pl.when(valid(k))
        def _(): ycp(k,True).start()
        k1=k-L
        @pl.when(valid(k1))
        def _():
            ycp(k1,False).wait_recv()
            xcp(k1,True).start()
        k2=k-2*L
        @pl.when(valid(k2))
        def _():
            xcp(k2,False).wait_recv()
            ccp(k2,True).start()
        k3=k-3*L
        @pl.when(valid(k3))
        def _(): ccp(k3,False).wait_recv()
        return 0
    lax.fori_loop(0,total,body,0)
    def drain(k,_):
        for d in range(Z-1):
            @pl.when(has_up&(z>=d))
            def _(): upc(d,k).wait_send()
            @pl.when(has_dn&(z+d<=Z-1))
            def _(): dnc(d,k).wait_send()
        ycp(k,True).wait_send(); xcp(k,True).wait_send(); ccp(k,True).wait_send()
        return 0
    lax.fori_loop(0,n,drain,0)

def gather(shard, Z, rc, L, cid):
    R=shard.shape[0]; n=R//rc; W=shard.shape[1]
    S=pltpu.SemaphoreType.DMA
    return pl.pallas_call(functools.partial(gather_kernel,Z,R,rc,L),
        out_shape=jax.ShapeDtypeStruct((Z,2,2,R,W),shard.dtype),
        in_specs=[pl.BlockSpec(memory_space=pl.ANY)], out_specs=pl.BlockSpec(memory_space=pl.ANY),
        scratch_shapes=[pltpu.VMEM((R,W),shard.dtype),S((2,)),S((Z-1,n)),S((Z-1,n)),S((Z-1,n)),S((Z-1,n)),S((n,)),S((n,)),S((n,)),S((n,)),S((n,)),S((n,))],
        compiler_params=pltpu.CompilerParams(collective_id=cid,has_side_effects=True))(shard)


def reduce_kernel(Z, T, L, segs, nx, ny, no, *refs):
    xs=refs[:nx]; ys=refs[nx:nx+ny]; outs=refs[nx+ny:nx+ny+no]
    (xbuf, ybuf, keep, s0, r0, s1, r1, s2, r2, su, ru, sd, rd, sx, rx, own, e_buf,
     xsem, ysem, q0, p0, q1, p1, q2, p2, qu, pu, qd, pd, qx, px) = refs[nx+ny+no:]
    dp=lax.axis_index("dp"); s=lax.axis_index("seq")
    c=dp%2; y=(dp//2)%2; z=dp//4; h=s%2
    upd=(dp+4,s); dnd=(dp-4,s); yd=(dp+2-4*y,s); xd=(dp,s+1-2*h); cd=(dp+1-2*c,s)
    has_up=z<Z-1; has_dn=z>0
    n=sum(g[5] for g in segs)
    starts=[]; a=0
    for g in segs: starts.append(a); a+=g[5]
    def load_x(i):
        xi,pieces,*_=segs[i]
        off=0; res=[]
        for (c0,w) in pieces:
            res.append(pltpu.make_async_copy(xs[xi].at[:,c0:c0+w], xbuf.at[i%2,:,off:off+w], xsem.at[i%2,len(res)])); off+=w
        return res
    def load_y(i,k):
        _,_,yi,c0,wide,cnt,_,_=segs[i]
        w=16384//wide
        return pltpu.make_async_copy(ys[yi].at[:,pl.ds(pl.multiple_of(c0+(k-starts[i])*w,128),w)], ybuf.at[k%2,:,0:w], ysem.at[k%2])
    def each(k,fn):
        for i in range(len(segs)):
            @pl.when((k>=starts[i])&(k<starts[i]+segs[i][5]))
            def _(): fn(i)
    for q in load_x(0): q.start()
    load_y(0,0).start()
    bar=pltpu.get_barrier_semaphore()
    @pl.when(has_up)
    def _(): pl.semaphore_signal(bar,inc=1,device_id=upd,device_id_type=MESHID)
    @pl.when(has_dn)
    def _(): pl.semaphore_signal(bar,inc=1,device_id=dnd,device_id_type=MESHID)
    for t in (yd,xd,cd): pl.semaphore_signal(bar,inc=1,device_id=t,device_id_type=MESHID)
    pl.semaphore_wait(bar,5-(z==0).astype(jnp.int32)-(z==Z-1).astype(jnp.int32))
    def rcopy(src,dst,ss,rs,dev): return pltpu.make_async_remote_copy(src,dst,ss,rs,device_id=dev,device_id_type=MESHID)
    NS=s0.shape[0]
    def c0(k): return rcopy(s0.at[k%NS],r0.at[k],q0.at[k%NS],p0.at[k],cd)
    def c1(k): return rcopy(s1.at[k%NS],r1.at[k],q1.at[k%NS],p1.at[k],xd)
    def c2(k): return rcopy(s2.at[k%NS],r2.at[k],q2.at[k%NS],p2.at[k],yd)
    def cu(k,j): return rcopy(su.at[k%NS,j],ru.at[k,j],qu.at[k%NS,j],pu.at[k,j],upd)
    def cdn(k,j): return rcopy(sd.at[k%NS,j],rd.at[k,j],qd.at[k%NS,j],pd.at[k,j],dnd)
    def cx(k): return rcopy(sx.at[k%NS],rx.at[k],qx.at[k%NS],px.at[k],xd)
    NE=e_buf.shape[0]; NK=keep.shape[0]
    mine=pl.ds(pl.multiple_of(h*32,32),32); other=pl.ds(pl.multiple_of((1-h)*32,32),32)
    def valid(k): return (k>=0)&(k<n)
    B1=L; B2=2*L; B3=3*L; BX=B3+(Z-1)*L+L; BF_=BX+L
    total=n+BF_
    def body(t,_):
        k=t
        @pl.when(valid(k))
        def _():
            def go(i):
                @pl.when(k==starts[i])
                def _():
                    for q in load_x(i): q.wait()
                    if i+1<len(segs):
                        for q in load_x(i+1): q.start()
                load_y(i,k).wait()
                @pl.when(k+1<starts[i]+segs[i][5])
                def _(): load_y(i,k+1).start()
                if i+1<len(segs):
                    @pl.when(k+1==starts[i]+segs[i][5])
                    def _(): load_y(i+1,k+1).start()
            each(k,go)
            @pl.when(k>=NS)
            def _(): c0(k-NS).wait_send()
            def comp(rr,par):
                cw=16384//rr
                r=lax.dot_general(xbuf[par,:,0:4*Z*rr],ybuf[k%2,:,0:cw],(((0,),(0,)),((),())),preferred_element_type=FL)
                r=r.astype(BF).reshape(Z,2,2,rr,cw)
                for cc in range(2):
                    @pl.when(c==cc)
                    def _():
                        for dst,part in ((keep.at[k%NK],r[:,:,cc]),(s0.at[k%NS],r[:,:,1-cc])):
                            if rr==128:
                                dst[:,:,:,0:128]=part[:,:,0:64]
                                dst[:,:,:,128:256]=part[:,:,64:128]
                            elif rr==64:
                                dst[...]=part
                            else:
                                dst[:,:,0:32,:]=part[:,:,:,0:256]
                                dst[:,:,32:64,:]=part[:,:,:,256:512]
            for par in range(2):
                for wide in (32,64,128):
                    conds=[(k>=starts[i])&(k<starts[i]+segs[i][5]) for i in range(len(segs)) if i%2==par and segs[i][4]==wide]
                    if conds:
                        cnd=functools.reduce(lambda a,b:a|b,conds)
                        @pl.when(cnd)
                        def _(): comp(wide,par)
            c0(k).start()
        k1=t-B1
        @pl.when(valid(k1))
        def _():
            c0(k1).wait_recv()
            @pl.when(k1>=NS)
            def _(): c1(k1-NS).wait_send()
            b=keep.at[k1%NK]
            s1[k1%NS]=(b[:,1-y,other,:].astype(FL)+r0[k1,:,1-y,other,:].astype(FL)).astype(BF)
            c1(k1).start()
            b[:,1-y,mine,:]=(b[:,1-y,mine,:].astype(FL)+r0[k1,:,1-y,mine,:].astype(FL)).astype(BF)
            e_buf[k1%NE]=(b[:,y].astype(FL)+r0[k1,:,y].astype(FL)).astype(BF)
        k2=t-B2
        @pl.when(valid(k2))
        def _():
            c1(k2).wait_recv()
            @pl.when(k2>=NS)
            def _(): c2(k2-NS).wait_send()
            s2[k2%NS]=(keep[k2%NK,:,1-y,mine,:].astype(FL)+r1[k2].astype(FL)).astype(BF)
            c2(k2).start()
        k3=t-B3
        @pl.when(valid(k3))
        def _():
            c2(k3).wait_recv()
            e_buf[k3%NE,:,mine,:]=(e_buf[k3%NE,:,mine,:].astype(FL)+r2[k3].astype(FL)).astype(BF)
        ku=t-B3-z*L
        @pl.when(valid(ku))
        def _():
            for j in range(Z):
                @pl.when((z==0)&(j>0))
                def _():
                    @pl.when(ku>=NS)
                    def _(): cu(ku-NS,j).wait_send()
                    su[ku%NS,j]=e_buf[ku%NE,j]
                    cu(ku,j).start()
                @pl.when((z>0)&(z<=j))
                def _(): cu(ku,j).wait_recv()
                @pl.when((z>0)&(z<j))
                def _():
                    @pl.when(ku>=NS)
                    def _(): cu(ku-NS,j).wait_send()
                    su[ku%NS,j]=(e_buf[ku%NE,j].astype(FL)+ru[ku,j].astype(FL)).astype(BF)
                    cu(ku,j).start()
        kd=t-B3-(Z-1-z)*L
        @pl.when(valid(kd))
        def _():
            for j in range(Z):
                @pl.when((z==Z-1)&(j<Z-1))
                def _():
                    @pl.when(kd>=NS)
                    def _(): cdn(kd-NS,j).wait_send()
                    sd[kd%NS,j]=e_buf[kd%NE,j]
                    cdn(kd,j).start()
                @pl.when((z<Z-1)&(z>=j))
                def _(): cdn(kd,j).wait_recv()
                @pl.when((z<Z-1)&(z>j))
                def _():
                    @pl.when(kd>=NS)
                    def _(): cdn(kd-NS,j).wait_send()
                    sd[kd%NS,j]=(e_buf[kd%NE,j].astype(FL)+rd[kd,j].astype(FL)).astype(BF)
                    cdn(kd,j).start()
        kx=t-BX
        @pl.when(valid(kx))
        def _():
            @pl.when(kx>=NS)
            def _(): cx(kx-NS).wait_send()
            for j in range(Z):
                @pl.when(z==j)
                def _():
                    v=e_buf[kx%NE,j].astype(FL)
                    if j>0: v=v+ru[kx,j].astype(FL)
                    if j<Z-1: v=v+rd[kx,j].astype(FL)
                    sx[kx%NS]=v.astype(BF)
            cx(kx).start()
        kf=t-BF_
        @pl.when(valid(kf))
        def _():
            cx(kf).wait_recv()
            v=sx[kf%NS].astype(FL)+rx[kf].astype(FL)
            def put(i):
                _,_,_,_,wide,cnt,oi,r0_=segs[i]
                j=kf-starts[i]
                row,col=r0_
                def cs(at,w): return pl.ds(pl.multiple_of(col+j*(16384//wide)+at,128),w)
                if wide==128:
                    outs[oi][row:row+64,cs(0,128)]=v[:,0:128]
                    outs[oi][row+64:row+128,cs(0,128)]=v[:,128:256]
                elif wide==64:
                    outs[oi][row:row+64,cs(0,256)]=v
                else:
                    outs[oi][row:row+32,cs(0,256)]=v[0:32]
                    outs[oi][row:row+32,cs(256,256)]=v[32:64]
            each(kf,put)
        return 0
    lax.fori_loop(0,total,body,0)
    def drain(k,_):
        c0(k).wait_send(); c1(k).wait_send(); c2(k).wait_send(); cx(k).wait_send()
        for j in range(Z):
            @pl.when(has_up&(z<j))
            def _(): cu(k,j).wait_send()
            @pl.when(has_dn&(z>j))
            def _(): cdn(k,j).wait_send()
        return 0
    lax.fori_loop(max(n-NS,0),n,drain,0)

def reduce_grads(xs, ys, segs, outshapes, Z, L, cid):
    T=xs[0].shape[0]
    n=sum(g[5] for g in segs)
    NS=4; NK=2*L+2; NE=(Z+3)*L+2
    S=pltpu.SemaphoreType.DMA
    V=pltpu.VMEM
    npc=max(len(g[1]) for g in segs)
    xw=max(sum(w for _,w in g[1]) for g in segs); yw=max(16384//g[4] for g in segs)
    scratch=[V((2,T,xw),BF),V((2,T,yw),BF),V((NK,Z,2,64,256),BF),
        V((NS,Z,2,64,256),BF),V((n,Z,2,64,256),BF), V((NS,Z,32,256),BF),V((n,Z,32,256),BF), V((NS,Z,32,256),BF),V((n,Z,32,256),BF),
        V((NS,Z,64,256),BF),V((n,Z,64,256),BF),V((NS,Z,64,256),BF),V((n,Z,64,256),BF),V((NS,64,256),BF),V((n,64,256),BF),V((8,128),FL),V((NE,Z,64,256),BF),
        S((2,npc)),S((2,)),S((NS,)),S((n,)),S((NS,)),S((n,)),S((NS,)),S((n,)),S((NS,Z)),S((n,Z)),S((NS,Z)),S((n,Z)),S((NS,)),S((n,))]
    return pl.pallas_call(functools.partial(reduce_kernel,Z,T,L,segs,len(xs),len(ys),len(outshapes)),
        out_shape=[jax.ShapeDtypeStruct(o,FL) for o in outshapes],
        in_specs=[pl.BlockSpec(memory_space=pl.ANY)]*(len(xs)+len(ys)),
        out_specs=[pl.BlockSpec(memory_space=pltpu.VMEM)]*len(outshapes),
        scratch_shapes=scratch,
        compiler_params=pltpu.CompilerParams(collective_id=cid,has_side_effects=True,vmem_limit_bytes=64*1024*1024-65536))(*xs,*ys)
def segments(xi,yi,oi,dps,rows,xcols,ycols,oc=0):
    rr=min(rows,128)
    res=[]
    for q in range(rows//rr):
        pieces=((0,xcols),) if rr==rows else tuple((d*rows+q*rr,rr) for d in range(dps))
        res.append((xi,pieces,yi,0,rr,ycols*rr//16384,oi,(q*rr,oc)))
    return res


def dot(a,b,ca,cb): return lax.dot_general(a,b,(((ca,),(cb,)),((),())),preferred_element_type=FL)
def fwd_kernel(HD, qr, ko, kt, vo, vt, o_ref, lse_ref):
    lane=lax.broadcasted_iota(jnp.int32,(1,128),1)
    first=lane<HD
    q=qr[...]*jnp.asarray(HD**-0.5,BF)
    k=jnp.concatenate([ko[...],kt[...]],0); v=jnp.concatenate([vo[...],vt[...]],0)
    res=[]
    for hd in range(2):
        m=first if hd==0 else ~first
        qm=jnp.where(m,q,jnp.zeros_like(q))
        s=dot(qm,k,1,1)
        mx=jnp.max(s,-1,keepdims=True)
        p=jnp.exp(s-mx)
        l=jnp.sum(p,-1,keepdims=True)
        o=dot(p.astype(BF),v,1,0)/l
        res.append((o,mx+jnp.log(l)))
    o_ref[...]=jnp.where(first,res[0][0],res[1][0]).astype(BF)
    lse_ref[...]=jnp.where(first,res[0][1],res[1][1])
def att_fwd(q,ko,kt,vo,vt,HD=64):
    T,D=q.shape
    spec=pl.BlockSpec((T,128),lambda i:(0,i))
    return pl.pallas_call(functools.partial(fwd_kernel,HD),grid=(D//128,),in_specs=[spec]*5,out_specs=[spec,spec],
        out_shape=[jax.ShapeDtypeStruct((T,D),BF),jax.ShapeDtypeStruct((T,D),FL)],
        compiler_params=pltpu.CompilerParams(vmem_limit_bytes=56*1024*1024))(q,ko,kt,vo,vt)
def bwd_kernel(HD, qr, ko, kt, vo, vt, o_ref, lse_ref, g_ref, dq_ref, dko, dkt, dvo, dvt):
    T=qr.shape[0]
    lane=lax.broadcasted_iota(jnp.int32,(1,128),1)
    first=lane<HD
    sc=HD**-0.5
    q=qr[...]*jnp.asarray(sc,BF)
    k=jnp.concatenate([ko[...],kt[...]],0); v=jnp.concatenate([vo[...],vt[...]],0)
    g=g_ref[...]
    go=g.astype(FL)*o_ref[...].astype(FL)
    lse=lse_ref[...]
    dqs=[]; dk=None
    for hd in range(2):
        m=first if hd==0 else ~first
        qm=jnp.where(m,q,jnp.zeros_like(q)); gm=jnp.where(m,g,jnp.zeros_like(g))
        delta=jnp.sum(jnp.where(m,go,0.0),-1,keepdims=True)
        ls=lse[:,hd*HD:hd*HD+1]
        s=dot(qm,k,1,1)
        p=jnp.exp(s-ls)
        dp=dot(gm,v,1,1)
        ds=(p*(dp-delta)).astype(BF)
        pb=p.astype(BF)
        dvv=dot(pb,gm,0,0)
        dkk=dot(ds,qm,0,0)
        dqs.append(dot(ds,k,1,0))
        if dk is None: dk,dv=dkk,dvv
        else: dk=dk+dkk; dv=dv+dvv
    dq_ref[...]=(jnp.where(first,dqs[0],dqs[1])*sc).astype(BF)
    dko[...]=dk[:T]; dkt[...]=dk[T:].astype(BF)
    dvo[...]=dv[:T]; dvt[...]=dv[T:].astype(BF)
def att_bwd(q,ko,kt,vo,vt,o,lse,g,HD=64):
    T,D=q.shape
    spec=pl.BlockSpec((T,128),lambda i:(0,i))
    return pl.pallas_call(functools.partial(bwd_kernel,HD),grid=(D//128,),in_specs=[spec]*8,out_specs=[spec]*5,
        out_shape=[jax.ShapeDtypeStruct((T,D),t) for t in (BF,FL,BF,FL,BF)],
        compiler_params=pltpu.CompilerParams(vmem_limit_bytes=60*1024*1024))(q,ko,kt,vo,vt,o,lse,g)


def norm_apply(stream, gain, shift):
    centred = stream - jnp.mean(stream, -1, keepdims=True)
    variance = jnp.mean(centred * centred, -1, keepdims=True)
    return centred * lax.rsqrt(variance + EPSILON) * gain + shift


def mm(left, right):
    return jnp.dot(left, right, preferred_element_type=FL)


def mmt(left, right):
    return lax.dot_general(left, right, (((1,), (1,)), ((), ())), preferred_element_type=FL)


def on_device(
    dps,
    seqs,
    tokens,
    skipped,
    cotangent,
    merge_weight,
    merge_bias,
    first_gain,
    first_shift,
    project_in,
    project_out,
    project_bias,
    second_gain,
    second_shift,
    expand_weight,
    expand_bias,
    reduce_weight,
    reduce_bias,
):
    rows, width = tokens.shape
    depth = dps // 4
    hidden = expand_weight.shape[1]
    dp = lax.axis_index("dp")
    seq = lax.axis_index("seq")
    cross = []
    pair = []
    for d in range(dps):
        for s in range(seqs):
            if d % 2 != s % 2:
                cross.append((d * seqs + s, (d + (1 if s % 2 else -1)) * seqs + s + (1 if d % 2 else -1)))
            pair.append((d * seqs + s, (d ^ 1) * seqs + s))
    stays = (dp % 2) == (seq % 2)

    def swap(value):
        return jnp.where(stays, value, lax.ppermute(value, ("dp", "seq"), cross))

    def other_core(value):
        return lax.ppermute(value, ("dp", "seq"), pair)

    own_tokens, own_skipped, own_cot = tokens, skipped, cotangent
    tokens, skipped, cotangent = swap(tokens), swap(skipped), swap(cotangent)

    small_list = [merge_bias, first_gain, first_shift, project_bias, second_gain, second_shift, reduce_bias, expand_bias]
    small = jnp.concatenate(small_list)
    piece = merge_bias.shape[0]
    small = jnp.pad(small.reshape(1, -1), ((0, 31), (0, width - small.shape[0])))
    cols = lambda w: [w[:, i * width : (i + 1) * width] for i in range(w.shape[1] // width)]
    parts = [merge_weight, *cols(project_in), small, project_out, *cols(expand_weight), reduce_weight]
    shard = jnp.concatenate(parts, 0)
    bounds = [0]
    for p in parts:
        bounds.append(bounds[-1] + p.shape[0])
    gathered = gather(shard, depth, 32, 1, 0).reshape(dps, shard.shape[0], width)

    def whole(i):
        return gathered[:, bounds[i] : bounds[i + 1]].reshape(-1, width)

    merge_full = whole(0)
    w_q, w_k, w_v = whole(1), whole(2), whole(3)
    out_full = whole(5)
    w_exp = [whole(6 + i) for i in range(hidden // width)]
    reduce_full = whole(6 + hidden // width)
    sm = gathered[:, bounds[4]].astype(FL)
    vec = [sm[:, i * piece : (i + 1) * piece].reshape(-1) for i in range(7)]
    merge_offset, gain_one, shift_one, proj_offset, gain_two, shift_two, reduce_offset = vec
    expand_offset = sm[:, 7 * piece : 7 * piece + hidden // dps].reshape(-1)

    joined = jnp.concatenate([tokens, skipped], axis=1)
    stream = mm(joined, merge_full) + merge_offset
    normed_one = norm_apply(stream, gain_one, shift_one).astype(BF)
    keys = mm(normed_one, w_k).astype(BF)
    values = mm(normed_one, w_v).astype(BF)
    keys_t, values_t = other_core(keys), other_core(values)
    queries = mm(normed_one, w_q).astype(BF)
    attended, logsum = att_fwd(queries, keys, keys_t, values, values_t, HD)
    stream_two = stream + mm(attended, out_full) + proj_offset
    normed_two = norm_apply(stream_two, gain_two, shift_two).astype(BF)
    expand_full = jnp.concatenate(w_exp, 1)
    hidden_pre = mm(normed_two, expand_full) + expand_offset
    activated = jax.nn.gelu(hidden_pre, approximate=False).astype(BF)
    output = swap((stream_two + mm(activated, reduce_full) + reduce_offset).astype(BF))

    grad_out = cotangent.astype(FL)
    reduce_bias_grad = jnp.sum(grad_out, 0)
    grad_act = mmt(cotangent, reduce_full)
    _, gelu_back = jax.vjp(partial(jax.nn.gelu, approximate=False), hidden_pre)
    grad_pre = gelu_back(grad_act)[0].astype(BF)
    expand_bias_grad = jnp.sum(grad_pre.astype(FL), 0)
    grad_normed_two = mmt(grad_pre, expand_full)
    _, second_back = jax.vjp(norm_apply, stream_two, gain_two, shift_two)
    grad_rows_two, second_gain_grad, second_shift_grad = second_back(grad_normed_two)
    grad_stream_two = grad_out + grad_rows_two
    grad_branch = grad_stream_two.astype(BF)
    project_bias_grad = jnp.sum(grad_branch.astype(FL), 0)
    grad_attended = mmt(grad_branch, out_full).astype(BF)
    lag = 2 if depth <= 4 else 1
    per = lambda w: w.shape[0]
    reduce_weight_grad, expand_weight_grad, project_out_grad = reduce_grads(
        (activated, normed_two, attended),
        (cotangent, grad_pre, grad_branch),
        segments(0, 0, 0, dps, per(reduce_weight), hidden, width)
        + segments(1, 1, 1, dps, per(expand_weight), width, hidden)
        + segments(2, 2, 2, dps, per(project_out), width, width),
        [reduce_weight.shape, expand_weight.shape, project_out.shape],
        depth, lag, 1,
    )
    d_q, dk_own, dk_t, dv_own, dv_t = att_bwd(
        queries, keys, keys_t, values, values_t, attended, logsum, grad_attended, HD
    )
    d_k = (dk_own + other_core(dk_t).astype(FL)).astype(BF)
    d_v = (dv_own + other_core(dv_t).astype(FL)).astype(BF)
    grad_normed_one = mmt(d_q, w_q) + mmt(d_k, w_k) + mmt(d_v, w_v)
    _, first_back = jax.vjp(norm_apply, stream, gain_one, shift_one)
    grad_rows_one, first_gain_grad, first_shift_grad = first_back(grad_normed_one)
    grad_stream = (grad_stream_two + grad_rows_one).astype(BF)
    merge_bias_grad = jnp.sum(grad_stream.astype(FL), 0)
    back = swap(grad_stream)
    seg_in = []
    for i in range(3):
        seg_in += segments(0, i, 0, dps, per(project_in), width, width, i * width)
    project_in_grad, merge_weight_grad = reduce_grads(
        (normed_one, joined),
        (d_q, d_k, d_v, grad_stream),
        seg_in + segments(1, 3, 1, dps, per(merge_weight), 2 * width, width),
        [project_in.shape, merge_weight.shape],
        depth, lag, 2,
    )
    tokens_grad = mmt(back, merge_full[:width])
    skipped_grad = mmt(back, merge_full[width:])

    big = [merge_weight_grad, project_in_grad, project_out_grad, expand_weight_grad, reduce_weight_grad]
    if seqs > 2:
        groups = [list(range(h, seqs, 2)) for h in range(2)]
        big = lax.psum(big, "seq", axis_index_groups=groups)
    vectors = [merge_bias_grad, first_gain_grad, first_shift_grad, project_bias_grad, second_gain_grad, second_shift_grad, reduce_bias_grad]
    packed = jnp.concatenate([v.reshape(dps, -1) for v in vectors + [expand_bias_grad]], 1)
    summed = lax.psum(packed, ("dp", "seq"))
    mine = lax.dynamic_index_in_dim(summed, dp, 0, keepdims=False)
    sm_out = [mine[i * piece : (i + 1) * piece] for i in range(7)]
    return (
        output, tokens_grad, skipped_grad, *big,
        sm_out[0], sm_out[1], sm_out[2], sm_out[3], sm_out[4], sm_out[5], mine[7 * piece :], sm_out[6],
    )


def solution(mesh):
    rows = P(("dp", "seq"), None)
    two = P("dp", None)
    one = P("dp")
    return jax.shard_map(
        partial(on_device, mesh.shape["dp"], mesh.shape["seq"]),
        mesh=mesh,
        in_specs=(rows, rows, rows, two, one, one, one, two, two, one, one, one, two, one, two, one),
        out_specs=(rows, rows, rows, two, two, two, two, two, one, one, one, one, one, one, one, one),
        check_vma=False,
    )
```
